512 devices in a mesh: groups: 2 (over y), tp: 8 (over x, core), sp: 32 (over z).
Axes of the slice: x: 4, y: 2, z: 32, core: 2. Of those that a mesh axis runs over, the one named last changes fastest.
The devices are a block of a 4x8x32 slice.
Arguments:
- query_rows: bfloat16 [4, 2048, 4096], P('groups', ('sp', 'tp')), parts along dimension 0, may hold values from -100 to 100
- key_rows: bfloat16 [4, 2048, 4096], P('groups', ('sp', 'tp')), parts along dimension 0, may hold values from -4 to 4
- value_rows: bfloat16 [4, 2048, 4096], P('groups', ('sp', 'tp')), parts along dimension 0, may hold values from -6 to 6
- residual: bfloat16 [4, 2048, 2560], P('groups', 'sp', 'tp'), parts along dimension 0, may hold values from -100 to 100
- modulation: float32 [4, 2560], P(None, 'tp'), may hold values from -3 to 3
- out_weight: bfloat16 [2560, 4096], P('tp', 'sp'), may hold values from -0.375 to 0.375
- up_weight: bfloat16 [2560, 7168], P('sp', 'tp'), may hold values from -0.125 to 0.125
- down_weight: bfloat16 [2560, 7168], P('sp', 'tp'), may hold values from -0.0625 to 0.0625
Outputs:
- block_out: bfloat16 [4, 2048, 2560], P('groups', 'sp', 'tp'), parts along dimension 0
The draws below stay inside these ranges and needn't reach their ends.
There are 2 independent parts, one for each index of `groups`. The reference program is written for one: setup_inputs(seed, part) draws one part's arguments, and reference() takes and returns one part's arrays. A program takes and returns all parts, laid end to end along the dimension named above; an argument that names none is the same for every part. Nothing has to cross between parts.
All inputs are finite; a program needn't handle non-finite values.
Results may differ from the reference program's by a relative error of at most 0.0044.
Values may be sent and summed in bfloat16 or wider, within the bound.
A program may use at most 64 MiB of HBM per device.

```python
import math
import jax
import jax.numpy as jnp
from jax import lax

D = 2560
HEADS = 32
HEAD_FEATURES = 128
FF = 7168
MB = 2
INNER = 4096
SEQ = 2048


def attention_inputs(key):
    base_key = jax.random.fold_in(key, 7)
    key_one, key_two = jax.random.split(base_key, 2)
    keys_drawn = jax.random.truncated_normal(key_one, -4.0, 4.0, (MB, SEQ, INNER), jnp.float32)
    queries = 2.0 * jax.random.truncated_normal(key_two, -4.0, 4.0, (MB, SEQ, INNER), jnp.float32)
    keys_final = keys_drawn
    return (queries, keys_final)


def draw_query_rows(key, part):
    return attention_inputs(key)[0].astype(jnp.bfloat16)


def draw_key_rows(key, part):
    return attention_inputs(key)[1].astype(jnp.bfloat16)


def draw_residual(key, part):
    base_key = jax.random.fold_in(key, 29)
    key_one, key_two = jax.random.split(base_key, 2)
    rising = jnp.exp(jnp.linspace(0.0, math.log(3.0), D, dtype=jnp.float32))
    roughness = jnp.exp(jax.random.uniform(key_one, (D,), jnp.float32, -0.35, 0.35))
    columns = rising * roughness
    column_offset = 1.5 * rising
    drawn = jax.random.truncated_normal(key_two, -4.0, 4.0, (MB, SEQ, D), jnp.float32) * columns + column_offset
    return drawn.astype(jnp.bfloat16)


def steps_of(key, dims, pieces, low, high):
    loudness, own = 1.0, jax.random.fold_in(key, 6)
    for axis_at, shards_of in pieces:
        draws = jnp.exp(jax.random.uniform(jax.random.fold_in(own, axis_at), (shards_of,), jnp.float32, low / len(pieces), high / len(pieces)))
        loudness = loudness * jnp.repeat(draws, dims[axis_at] // shards_of).reshape([-1 if axis == axis_at else 1 for axis in range(len(dims))])
    return loudness


def noise(own_key, shape, scale, most, cuts=(), kind=jnp.bfloat16):
    level = steps_of(own_key, shape, cuts, -0.22, 0.18) if cuts else 1.0
    values = jax.random.normal(own_key, shape, jnp.float32) * scale * level
    return jnp.minimum(jnp.maximum(values, -most), most).astype(kind)


def setup_inputs(seed: int = 0, part: int = 0) -> dict:
    streams_of = jax.random.split(jax.random.key(seed), 9)
    own_keys = jax.random.split(jax.random.fold_in(streams_of[8], part), 9)
    query_rows = draw_query_rows(jax.random.fold_in(jax.random.fold_in(streams_of[8], part), 71), part)
    key_rows = draw_key_rows(jax.random.fold_in(jax.random.fold_in(streams_of[8], part), 71), part)
    value_rows = noise(own_keys[2], (MB, SEQ, INNER), 1.0, 6.0, ((1, 256),))
    residual = draw_residual(jax.random.fold_in(jax.random.fold_in(streams_of[8], part), 71), part)
    modulation = noise(streams_of[4], (4, D), 0.6, 3.0, ((1, 8),), jnp.float32)
    out_weight = noise(streams_of[5], (D, INNER), (INNER // 16) ** -0.5, 0.375, ((0, 8), (1, 32)))
    up_weight = noise(streams_of[6], (D, FF), D ** -0.5, 0.125, ((0, 32), (1, 8)))
    down_weight = noise(streams_of[7], (D, FF), FF ** -0.5, 0.0625, ((0, 32), (1, 8)))
    return dict(query_rows=query_rows, key_rows=key_rows, value_rows=value_rows, residual=residual, modulation=modulation, out_weight=out_weight, up_weight=up_weight, down_weight=down_weight)


def one_head(blocks):
    block_queries, block_keys, block_values = blocks
    attention_logits = jnp.einsum('rzs,ros->rzo', block_queries.astype(jnp.float32), block_keys.astype(jnp.float32)) / math.sqrt(HEAD_FEATURES)
    highest = lax.optimization_barrier(jnp.max(attention_logits, axis=-1, keepdims=True))
    exponent = jnp.exp(attention_logits - highest)
    row_total = lax.optimization_barrier(jnp.sum(exponent, axis=-1, keepdims=True))
    attention_weights = exponent.astype(jnp.bfloat16)
    weighted_values = jnp.einsum('ezh,ehu->ezu', attention_weights.astype(jnp.float32), block_values.astype(jnp.float32))
    return (weighted_values / row_total).astype(jnp.bfloat16)

def split_heads(packed):
    return jnp.transpose(packed.reshape(MB, SEQ, HEADS, HEAD_FEATURES), (2, 0, 1, 3))

def reference(query_rows, key_rows, value_rows, residual, modulation, out_weight, up_weight, down_weight):
    heads_out = lax.map(one_head, (split_heads(query_rows), split_heads(key_rows), split_heads(value_rows)))
    attended = jnp.transpose(heads_out, (1, 2, 0, 3)).reshape(MB * SEQ, INNER)
    projected = jnp.dot(attended, out_weight.T, preferred_element_type=jnp.float32)
    mixed_rows = residual.reshape(MB * SEQ, D).astype(jnp.float32) + modulation[0] * projected
    row_mean = lax.optimization_barrier(jnp.mean(mixed_rows, axis=1, keepdims=True))
    spread = lax.optimization_barrier(jnp.mean(jnp.square(mixed_rows - row_mean), axis=1, keepdims=True))
    normed = ((mixed_rows - row_mean) * lax.rsqrt(spread + 1e-06) * (1.0 + modulation[2]) + modulation[1]).astype(jnp.bfloat16)
    hidden = jnp.dot(normed, up_weight, preferred_element_type=jnp.float32)
    active = jax.nn.gelu(hidden, approximate=True).astype(jnp.bfloat16)
    down_out = jnp.dot(active, down_weight.T, preferred_element_type=jnp.float32)
    return (mixed_rows + modulation[3] * down_out).astype(jnp.bfloat16).reshape(MB, SEQ, D)
```

```python
import functools
import math

import jax
import jax.numpy as jnp
from jax import lax
from jax.experimental import pallas as pl
from jax.experimental.pallas import tpu as pltpu
from jax.sharding import PartitionSpec as P

MESH = pl.DeviceIdType.MESH
F32 = jnp.float32
BF16 = jnp.bfloat16


def dot_last(a, b):
    return lax.dot_general(a, b, (((1,), (1,)), ((), ())), preferred_element_type=F32)


def dot(a, b):
    return jnp.dot(a, b, preferred_element_type=F32)


def kernel(
    sp, tp, q_hbm, k_hbm, v_hbm, res_ref, mod_ref, wo_hbm, up_hbm, dn_hbm, out_ref,
    qkv, qkvr, kvo, qp, kp, vp, scores, att, att_all, wo_full, w2, mixed, stats, normed_all,
    active, part_send, part_recv,
    local_sem, ring_recv, ring_send, pair_sem, far_sem, a2a_sem, kv_sem, back_sem, gat_sem, gnm_sem, st_sem, rs_sem,
):
    heads, feats = sp, qkvr.shape[-1]
    nx = tp // 2
    g, t, z = lax.axis_index("groups"), lax.axis_index("tp"), lax.axis_index("sp")
    x, c = t // 2, t % 2
    par = g % 2
    xr, xl, xo = (x + 1) % nx, (x + nx - 1) % nx, (x + 2) % nx
    zr, zl = (z + 1) % sp, (z + sp - 1) % sp
    sib = t + 1 - 2 * c
    pending = []

    def remote(src, dst, send, recv, dev):
        return pltpu.make_async_remote_copy(
            src_ref=src, dst_ref=dst, send_sem=send, recv_sem=recv, device_id=dev, device_id_type=MESH
        )

    def send(src, dst, s, r, dev):
        d = remote(src, dst, s, r, dev)
        d.start()
        pending.append(d)

    shard = up_hbm.shape[0]

    def w2rows(a, o):
        return w2.at[a, pl.ds(pl.multiple_of(o * shard, 16), shard), :]

    locals_w = [
        pltpu.make_async_copy(wo_hbm, wo_full.at[z], local_sem.at[0]),
        pltpu.make_async_copy(up_hbm, w2rows(0, z), local_sem.at[1]),
        pltpu.make_async_copy(dn_hbm, w2rows(1, z), local_sem.at[2]),
    ]
    locals_a = [
        pltpu.make_async_copy(r, qkv.at[i], local_sem.at[3 + i]) for i, r in enumerate((q_hbm, k_hbm, v_hbm))
    ]
    for d in locals_w + locals_a:
        d.start()

    bar = pltpu.get_barrier_semaphore()
    near = [{"tp": (t + j) % tp} for j in range(1, tp)]
    near += [{"sp": zz, "tp": 2 * x + cc} for zz in (zr, zl) for cc in (0, 1)]
    near += [{"groups": g + 1 - 2 * par}]
    for dev in near:
        pl.semaphore_signal(bar, inc=1, device_id=dev, device_id_type=MESH)
    pl.semaphore_wait(bar, len(near))

    hops = ((sp // 2 - 1, sp // 2), (sp // 2, sp // 2 - 1))

    def ring_ref(a, o):
        return wo_full.at[o] if a == 0 else w2rows(par, o)

    def ring_copy(a, d, k):
        o = (z - k + sp) % sp if d == 0 else (z + k) % sp
        return remote(
            ring_ref(a, o), ring_ref(a, o), ring_send.at[2 * a + d], ring_recv.at[2 * a + d, k],
            {"sp": zr if d == 0 else zl},
        )

    def ring_arrival(a, d, k):
        o = (z - 1 - k + 2 * sp) % sp if d == 0 else (z + 1 + k) % sp
        ref = ring_ref(a, o)
        return remote(ref, ref, ring_send.at[2 * a + d], ring_recv.at[2 * a + d, k], {"sp": zr if d == 0 else zl}), o

    def push(o):
        remote(w2rows(par, o), w2rows(par, o), pair_sem.at[0], pair_sem.at[1], {"groups": g + 1 - 2 * par}).start()

    def ring_step(a, k):
        for d in (0, 1):
            if k >= 1 and k - 1 < hops[a][d]:
                arrival, o = ring_arrival(a, d, k - 1)
                arrival.wait_recv()
                if a == 1:
                    push(o)
            if k < hops[a][d]:
                ring_copy(a, d, k).start()

    last = sp // 2
    done = [0, 0]

    def advance(n_wo=0, n_w2=0):
        for i in range(max(n_wo, n_w2)):
            for a, n in ((0, n_wo), (1, n_w2)):
                if i < n and done[a] <= last:
                    ring_step(a, done[a])
                    done[a] += 1

    for d in locals_w:
        d.wait()
    advance(1, 1)
    for d in locals_a:
        d.wait()

    slot = 2 * z + c

    def head_cols(h):
        return pl.ds(pl.multiple_of(h * feats, 128), feats)

    def send_heads(e):
        zz = (z + e + sp) % sp
        for m in (0, 1):
            remote(
                qkv.at[:, m, :, head_cols(zz)], qkvr.at[:, slot], a2a_sem.at[0], a2a_sem.at[1],
                {"sp": zz, "tp": 2 * x + m},
            ).start()

    def send_both(lo, hi):
        def one(e, carry):
            send_heads(e)
            send_heads(-e)
            return carry
        lax.fori_loop(lo, hi, one, 0)

    remote(
        qkv.at[:, 1 - c, :, head_cols(z)], qkvr.at[:, slot], a2a_sem.at[0], a2a_sem.at[1], {"tp": sib}
    ).start()
    qkvr[:, slot] = qkv[:, c, :, head_cols(z)]
    send_both(1, 2)
    reach, r = 1, 0
    while reach < sp // 2:
        for zz in ((z + reach) % sp, (z - reach + sp) % sp):
            pl.semaphore_signal(far_sem.at[r], inc=1, device_id={"sp": zz}, device_id_type=MESH)
        pl.semaphore_wait(far_sem.at[r], 2)
        send_both(reach + 1, min(2 * reach, sp // 2 - 1) + 1)
        reach, r = 2 * reach, r + 1
        advance(1, 0)
    send_heads(sp // 2)
    advance(0, 1)
    n = 2 * sp
    rest = qkvr.at[:, pl.ds(0, n - 1)]
    pltpu.make_async_copy(rest, rest, a2a_sem.at[1]).wait()

    own_kv = qkvr.at[pl.ds(1, 2)]
    right, left = {"tp": 2 * xr + c}, {"tp": 2 * xl + c}
    send(own_kv, kvo.at[0], kv_sem.at[0], kv_sem.at[4], right)
    send(own_kv, kvo.at[1], kv_sem.at[1], kv_sem.at[5], left)
    advance(1, 1)

    def pack(ref):
        v = ref[...].astype(F32)
        return v.reshape(v.shape[0] * v.shape[1], v.shape[2]).astype(BF16)

    rows = 8 * n
    qp[...] = pack(qkvr.at[0])
    kp[pl.ds(0, rows), :] = pack(qkvr.at[1])
    vp[pl.ds(0, rows), :] = pack(qkvr.at[2])
    remote(own_kv, kvo.at[0], kv_sem.at[0], kv_sem.at[4], right).wait_recv()
    send(kvo.at[0, 0], kvo.at[2, 0], kv_sem.at[2], kv_sem.at[6], right)
    remote(own_kv, kvo.at[1], kv_sem.at[1], kv_sem.at[5], left).wait_recv()
    send(kvo.at[1, 1], kvo.at[2, 1], kv_sem.at[3], kv_sem.at[7], left)
    for j in (0, 1):
        kp[pl.ds((1 + j) * rows, rows), :] = pack(kvo.at[j, 0])
        vp[pl.ds((1 + j) * rows, rows), :] = pack(kvo.at[j, 1])
    advance(1, 1)
    remote(kvo.at[0, 0], kvo.at[2, 0], kv_sem.at[2], kv_sem.at[6], right).wait_recv()
    remote(kvo.at[1, 1], kvo.at[2, 1], kv_sem.at[3], kv_sem.at[7], left).wait_recv()
    kp[pl.ds(3 * rows, rows), :] = pack(kvo.at[2, 0])
    vp[pl.ds(3 * rows, rows), :] = pack(kvo.at[2, 1])

    scale = 1.0 / math.sqrt(feats)
    qb = 128

    def attend(i, carry):
        q = qp[pl.ds(pl.multiple_of(i * qb, qb), qb), :]
        high = None
        for j in range(nx):
            s = dot_last(q, kp[j * rows : (j + 1) * rows, :])
            scores[:, j * rows : (j + 1) * rows] = s
            top = jnp.max(s, axis=1, keepdims=True)
            high = top if high is None else jnp.maximum(high, top)
        total = jnp.zeros((qb, 1), F32)
        acc = jnp.zeros((qb, feats), F32)
        for j in range(nx):
            e = jnp.exp((scores[:, j * rows : (j + 1) * rows] - high) * scale)
            total += jnp.sum(e, axis=1, keepdims=True)
            acc += dot(e.astype(BF16), vp[j * rows : (j + 1) * rows, :])
        o = acc / total
        att[pl.ds(i * (qb // 8), qb // 8)] = o.reshape(qb // 8, 8, feats).astype(BF16)
        return carry

    lax.fori_loop(0, rows // qb, attend, 0)
    advance(2, 1)

    def send_back(zz, cc):
        return remote(
            att.at[2 * zz + cc], att_all.at[c, 2 * x + cc, :, head_cols(z)], back_sem.at[0], back_sem.at[1],
            {"sp": zz, "tp": 2 * x + cc},
        )

    def back_one(e, carry):
        zz = (z + e) % sp
        send_back(zz, 0).start()
        send_back(zz, 1).start()
        return carry

    lax.fori_loop(1, sp, back_one, 0)
    remote(
        att.at[2 * z + 1 - c], att_all.at[c, sib, :, head_cols(z)], back_sem.at[0], back_sem.at[1], {"tp": sib}
    ).start()
    att_all[c, t, :, head_cols(z)] = att[slot]
    advance(4, 2)
    most = att.at[pl.ds(0, n - 1)]
    pltpu.make_async_copy(most, most, back_sem.at[1]).wait()

    def tp_gather(full, half, sems, between):
        rs = lambda i: sems.at[1, i]
        ss = lambda i: sems.at[0, i]
        tl, tr, to = 2 * xl + c, 2 * xr + c, 2 * xo + c
        sibling = {"tp": sib}

        def got(ref, i):
            remote(ref, ref, ss(i), rs(i), sibling).wait_recv()

        send(full(t), full(t), ss(0), rs(0), right)
        send(full(t), full(t), ss(1), rs(1), left)
        send(full(t), full(t), ss(2), rs(2), sibling)
        between()
        got(full(tl), 0)
        send(half(tl, 0), half(tl, 0), ss(3), rs(3), right)
        send(full(tl), full(tl), ss(4), rs(4), sibling)
        got(full(tr), 1)
        send(half(tr, 1), half(tr, 1), ss(5), rs(5), left)
        send(full(tr), full(tr), ss(6), rs(6), sibling)
        got(half(to, 0), 3)
        send(half(to, 0), half(to, 0), ss(7), rs(7), sibling)
        got(half(to, 1), 5)
        send(half(to, 1), half(to, 1), ss(8), rs(8), sibling)
        d = 1 - 2 * c
        got(full(t + d), 2)
        got(full(tl + d), 4)
        got(full(tr + d), 6)
        got(half(to + d, 0), 7)
        got(half(to + d, 1), 8)

    tp_gather(lambda i: att_all.at[:, i], lambda i, h: att_all.at[h, i], gat_sem, lambda: advance(2, 1))
    advance(sp, 0)

    nrow, width = mixed.shape
    mixed[...] = jnp.zeros_like(mixed)

    def project(i, carry):
        acc = jnp.zeros((nrow, width), F32)
        for u in range(4):
            h = i * 4 + u
            a = att_all[:, :, :, head_cols(h)].astype(F32).reshape(nrow, feats).astype(BF16)
            acc += dot_last(a, wo_full[h])
        mixed[...] += acc
        return carry

    lax.fori_loop(0, heads // 4, project, 0)
    res = res_ref[...].astype(F32).reshape(nrow, width)
    mix = res + mod_ref[0:1, :] * mixed[...]
    mixed[...] = mix
    local_sum = jnp.sum(mix, axis=1, keepdims=True)
    off = mix - local_sum * (1.0 / width)
    local_sq = jnp.sum(off * off, axis=1, keepdims=True)

    def as_row(col):
        return jnp.transpose(jnp.broadcast_to(col, (nrow, nrow)))[0:4, :]

    stats[t] = jnp.concatenate([as_row(local_sum), as_row(local_sq)], axis=0)
    advance(0, 1)
    for j in range(1, tp):
        dev = (t + j) % tp
        remote(stats.at[t], stats.at[t], st_sem.at[0], st_sem.at[1], {"tp": dev}).start()
    others = stats.at[pl.ds(0, tp - 1)]
    pltpu.make_async_copy(others, others, st_sem.at[1]).wait()
    every = stats[...]
    sums, squares = every[:, 0:1, :], every[:, 4:5, :]
    mean = jnp.sum(sums, axis=0) * (1.0 / (tp * width))
    shift = sums * (1.0 / width) - mean[None]
    spread = (jnp.sum(squares, axis=0) + width * jnp.sum(shift * shift, axis=0)) * (1.0 / (tp * width))
    inv = lax.rsqrt(spread + 1e-06)

    def as_col(row):
        return jnp.transpose(jnp.broadcast_to(row, (nrow, nrow)))[:, 0:1]

    mix = mixed[...]
    normed = (mix - as_col(mean)) * as_col(inv) * (1.0 + mod_ref[2:3, :]) + mod_ref[1:2, :]
    normed_all[t] = normed.astype(BF16)
    advance(0, 1)
    hr = nrow // 2
    tp_gather(
        lambda i: normed_all.at[i], lambda i, h: normed_all.at[i, pl.ds(h * hr, hr), :], gnm_sem, lambda: advance(0, 1)
    )
    advance(0, sp)
    pushed = w2.at[1 - par, pl.ds(0, (sp - 1) * shard), :]
    pltpu.make_async_copy(pushed, pushed, pair_sem.at[1]).wait()

    ff = active.shape[1]
    for lo in range(0, ff, 256):
        hi = min(lo + 256, ff)
        acc = jnp.zeros((nrow, hi - lo), F32)
        for i in range(tp):
            acc += dot(normed_all[i], w2[0, i * width : (i + 1) * width, lo:hi])
        inner = math.sqrt(2 / math.pi) * (acc + 0.044715 * (acc * acc * acc))
        active[:, lo:hi] = (0.5 * acc * (1.0 + jnp.tanh(inner))).astype(BF16)

    def down(i):
        dev = (t + i) % tp
        block = w2[1, pl.ds(pl.multiple_of(dev * width, 16), width), :]
        return dev, dot_last(active[...], block).astype(BF16)

    waiting = None
    for i in (4, 5, 3, 2, 6, 7, 1, 0):
        dev, block = down(i)
        if i:
            part_send[dev] = block
        else:
            part_recv[t] = block
        if waiting is not None:
            remote(part_send.at[waiting], part_recv.at[t], rs_sem.at[0], rs_sem.at[1], {"tp": waiting}).start()
        waiting = dev
    seven = part_recv.at[pl.ds(0, tp - 1)]
    pltpu.make_async_copy(seven, seven, rs_sem.at[1]).wait()
    total = part_recv[0].astype(F32)
    for i in range(1, tp):
        total += part_recv[i].astype(F32)
    out = mixed[...] + mod_ref[3:4, :] * total
    out_ref[...] = out.astype(BF16).reshape(out_ref.shape)

    for d in pending:
        d.wait_send()
    pltpu.make_async_copy(rest, rest, a2a_sem.at[0]).wait()
    pltpu.make_async_copy(most, most, back_sem.at[0]).wait()
    pltpu.make_async_copy(others, others, st_sem.at[0]).wait()
    pltpu.make_async_copy(seven, seven, rs_sem.at[0]).wait()
    pltpu.make_async_copy(pushed, pushed, pair_sem.at[0]).wait()
    for a in (0, 1):
        for d in (0, 1):
            k = hops[a][d]
            ref = wo_full.at[pl.ds(0, k)] if a == 0 else w2.at[par, pl.ds(0, k * shard), :]
            pltpu.make_async_copy(ref, ref, ring_send.at[2 * a + d]).wait()


def block(sp, tp, q, k, v, residual, modulation, wo, up, dn):
    mb, tokens, inner = q.shape
    feats = inner // sp
    width = wo.shape[0]
    nrow = mb * residual.shape[1]
    shard, ff = up.shape
    nslot = 2 * sp
    rows = tokens * nslot
    dma, reg = pltpu.SemaphoreType.DMA, pltpu.SemaphoreType.REGULAR
    anyspace = pl.BlockSpec(memory_space=pl.ANY)
    vmem = pl.BlockSpec(memory_space=pltpu.VMEM)
    V = pltpu.VMEM
    return pl.pallas_call(
        functools.partial(kernel, sp, tp),
        out_shape=jax.ShapeDtypeStruct(residual.shape, BF16),
        in_specs=[anyspace] * 3 + [vmem] * 2 + [anyspace] * 3,
        out_specs=vmem,
        scratch_shapes=[
            V((3, mb, tokens, inner), BF16),
            V((3, nslot, tokens, feats), BF16),
            V((3, 2, nslot, tokens, feats), BF16),
            V((rows, feats), BF16),
            V((tp // 2 * rows, feats), BF16),
            V((tp // 2 * rows, feats), BF16),
            V((128, tp // 2 * rows), F32),
            V((nslot, tokens, feats), BF16),
            V((mb, tp, tokens, inner), BF16),
            V((sp, width, feats), BF16),
            V((2, sp * shard, ff), BF16),
            V((nrow, width), F32),
            V((tp, 8, 128), F32),
            V((tp, nrow, width), BF16),
            V((nrow, ff), BF16),
            V((tp, nrow, width), BF16),
            V((tp, nrow, width), BF16),
            dma((6,)), dma((4, sp // 2)), dma((4,)), dma((2,)), reg((8,)), dma((2,)), dma((8,)), dma((2,)),
            dma((2, 9)), dma((2, 9)), dma((2,)), dma((2,)),
        ],
        compiler_params=pltpu.CompilerParams(
            collective_id=0, has_side_effects=True, vmem_limit_bytes=60 * 1024 * 1024
        ),
    )(q, k, v, residual, modulation, wo, up, dn)


def solution(mesh):
    in_specs = (
        P("groups", ("sp", "tp"), None),
        P("groups", ("sp", "tp"), None),
        P("groups", ("sp", "tp"), None),
        P("groups", "sp", "tp"),
        P(None, "tp"),
        P("tp", "sp"),
        P("sp", "tp"),
        P("sp", "tp"),
    )
    body = functools.partial(block, mesh.shape["sp"], mesh.shape["tp"])
    return jax.shard_map(body, mesh=mesh, in_specs=in_specs, out_specs=P("groups", "sp", "tp"), check_vma=False)
```

```python
import functools
import math

import jax
import jax.numpy as jnp
from jax import lax
from jax.experimental import pallas as pl
from jax.experimental.pallas import tpu as pltpu
from jax.sharding import PartitionSpec as P

MESH = pl.DeviceIdType.MESH
F32 = jnp.float32
BF16 = jnp.bfloat16


def dot_last(a, b):
    return lax.dot_general(a, b, (((1,), (1,)), ((), ())), preferred_element_type=F32)


def dot(a, b):
    return jnp.dot(a, b, preferred_element_type=F32)


def kernel(
    sp, tp, q_hbm, k_hbm, v_hbm, res_ref, mod_ref, wo_hbm, up_hbm, dn_hbm, out_ref,
    qkv, qkvr, kvo, qp, kp, vp, scores, att, att_all, wo_full, w2, mixed, stats, normed_all,
    active, part_send, part_recv,
    local_sem, ring_recv, ring_send, pair_sem, below_sem, hello_sem, a2a_sem, kv_sem, back_sem, gat_sem, gnm_sem, st_sem, rs_sem,
):
    heads, feats = sp, qkvr.shape[-1]
    nx = tp // 2
    g, t, z = lax.axis_index("groups"), lax.axis_index("tp"), lax.axis_index("sp")
    x, c = t // 2, t % 2
    par = g % 2
    xr, xl, xo = (x + 1) % nx, (x + nx - 1) % nx, (x + 2) % nx
    zr, zl = (z + 1) % sp, (z + sp - 1) % sp
    sib = t + 1 - 2 * c
    pending = []

    def remote(src, dst, send, recv, dev):
        return pltpu.make_async_remote_copy(
            src_ref=src, dst_ref=dst, send_sem=send, recv_sem=recv, device_id=dev, device_id_type=MESH
        )

    def send(src, dst, s, r, dev):
        d = remote(src, dst, s, r, dev)
        d.start()
        pending.append(d)

    shard = up_hbm.shape[0]

    def w2rows(a, o):
        return w2.at[a, pl.ds(pl.multiple_of(o * shard, 16), shard), :]

    locals_w = [
        pltpu.make_async_copy(wo_hbm, wo_full.at[z], local_sem.at[0]),
        pltpu.make_async_copy(up_hbm, w2rows(0, z), local_sem.at[1]),
        pltpu.make_async_copy(dn_hbm, w2rows(1, z), local_sem.at[2]),
    ]
    locals_a = [
        pltpu.make_async_copy(r, qkv.at[i], local_sem.at[3 + i]) for i, r in enumerate((q_hbm, k_hbm, v_hbm))
    ]
    for d in locals_w + locals_a:
        d.start()

    bar = pltpu.get_barrier_semaphore()
    beside = [{"tp": (t + j) % tp} for j in range(1, tp)] + [{"groups": g + 1 - 2 * par}]

    def greet(devs):
        for dev in devs:
            pl.semaphore_signal(bar, inc=1, device_id=dev, device_id_type=MESH)

    greet(beside)
    pl.when(z > 0)(lambda: greet([{"sp": zl, "tp": 2 * x + cc} for cc in (0, 1)]))
    pl.when(z < sp - 1)(lambda: greet([{"sp": zr, "tp": 2 * x + cc} for cc in (0, 1)]))
    pl.semaphore_wait(bar, len(beside) + 2 * jnp.minimum(z, 1) + 2 * jnp.minimum(sp - 1 - z, 1))

    pl.when(z > 0)(lambda: pl.semaphore_wait(below_sem.at[0], 1))

    @pl.when(z < sp - 1)
    def _():
        pl.semaphore_signal(below_sem.at[0], inc=1, device_id={"sp": zr}, device_id_type=MESH)

    def hello(zz, carry):
        pl.semaphore_signal(hello_sem.at[z], inc=1, device_id={"sp": zz}, device_id_type=MESH)
        return carry

    lax.fori_loop(0, z, hello, 0)

    hops = ((sp // 2 - 1, sp // 2), (sp // 2, sp // 2 - 1))

    def ring_ref(a, o):
        return wo_full.at[o] if a == 0 else w2rows(par, o)

    def ring_copy(a, d, k):
        o = (z - k + sp) % sp if d == 0 else (z + k) % sp
        return remote(
            ring_ref(a, o), ring_ref(a, o), ring_send.at[2 * a + d], ring_recv.at[2 * a + d, k],
            {"sp": zr if d == 0 else zl},
        )

    def ring_arrival(a, d, k):
        o = (z - 1 - k + 2 * sp) % sp if d == 0 else (z + 1 + k) % sp
        ref = ring_ref(a, o)
        return remote(ref, ref, ring_send.at[2 * a + d], ring_recv.at[2 * a + d, k], {"sp": zr if d == 0 else zl}), o

    def push(o):
        remote(w2rows(par, o), w2rows(par, o), pair_sem.at[0], pair_sem.at[1], {"groups": g + 1 - 2 * par}).start()

    def ring_part(a, k):
        for d in (0, 1):
            @pl.when(k - 1 < hops[a][d])
            def _():
                arrival, o = ring_arrival(a, d, k - 1)
                arrival.wait_recv()
                if a == 1:
                    push(o)

            @pl.when(k < hops[a][d])
            def _():
                ring_copy(a, d, k).start()

    half = sp // 2

    def ring_step(i, carry):
        pl.when(i <= half)(lambda: ring_part(0, i))
        pl.when((i > half) | (i % 2 == 0))(lambda: ring_part(1, jnp.where(i > half, i - half // 2, i // 2)))
        return carry

    last = half + half // 2
    at = [None]

    def advance(n=1, upto=0):
        end = jnp.minimum(jnp.maximum(at[0] + n, upto), last + 1)
        lax.fori_loop(at[0], end, ring_step, 0)
        at[0] = end

    def ring_start(d):
        ring_copy(0, d, 0).start()
        ring_copy(1, d, 0).start()

    for d in locals_w:
        d.wait()
    ring_start(0)
    pl.when(z > 0)(lambda: ring_start(1))
    for d in locals_a:
        d.wait()

    slot = 2 * z + c

    def head_cols(h):
        return pl.ds(pl.multiple_of(h * feats, 128), feats)

    def send_heads(e):
        zz = (z + e + sp) % sp
        for m in (0, 1):
            remote(
                qkv.at[:, m, :, head_cols(zz)], qkvr.at[:, slot], a2a_sem.at[0], a2a_sem.at[1],
                {"sp": zz, "tp": 2 * x + m},
            ).start()

    remote(
        qkv.at[:, 1 - c, :, head_cols(z)], qkvr.at[:, slot], a2a_sem.at[0], a2a_sem.at[1], {"tp": sib}
    ).start()
    qkvr[:, slot] = qkv[:, c, :, head_cols(z)]

    def down_one(e, carry):
        send_heads(-e)
        return carry

    def up_one(e, carry):
        pl.semaphore_wait(hello_sem.at[z + e], 1)
        send_heads(e)

        @pl.when((e % 2 == 0) & (e // 2 <= z))
        def _():
            ring_step(e // 2, 0)

        return carry

    lax.fori_loop(1, z + 1, down_one, 0)
    lax.fori_loop(1, sp - z, up_one, 0)
    pl.when(z == 0)(lambda: ring_start(1))
    at[0] = 1 + jnp.minimum((sp - 1 - z) // 2, z)
    advance(1)
    n = 2 * sp
    rest = qkvr.at[:, pl.ds(0, n - 1)]
    pltpu.make_async_copy(rest, rest, a2a_sem.at[1]).wait()

    own_kv = qkvr.at[pl.ds(1, 2)]
    right, left = {"tp": 2 * xr + c}, {"tp": 2 * xl + c}
    send(own_kv, kvo.at[0], kv_sem.at[0], kv_sem.at[4], right)
    send(own_kv, kvo.at[1], kv_sem.at[1], kv_sem.at[5], left)
    advance(2)

    def pack(ref):
        v = ref[...].astype(F32)
        return v.reshape(v.shape[0] * v.shape[1], v.shape[2]).astype(BF16)

    rows = 8 * n
    qp[...] = pack(qkvr.at[0])
    kp[pl.ds(0, rows), :] = pack(qkvr.at[1])
    vp[pl.ds(0, rows), :] = pack(qkvr.at[2])
    remote(own_kv, kvo.at[0], kv_sem.at[0], kv_sem.at[4], right).wait_recv()
    send(kvo.at[0, 0], kvo.at[2, 0], kv_sem.at[2], kv_sem.at[6], right)
    remote(own_kv, kvo.at[1], kv_sem.at[1], kv_sem.at[5], left).wait_recv()
    send(kvo.at[1, 1], kvo.at[2, 1], kv_sem.at[3], kv_sem.at[7], left)
    for j in (0, 1):
        kp[pl.ds((1 + j) * rows, rows), :] = pack(kvo.at[j, 0])
        vp[pl.ds((1 + j) * rows, rows), :] = pack(kvo.at[j, 1])
    advance(2)
    remote(kvo.at[0, 0], kvo.at[2, 0], kv_sem.at[2], kv_sem.at[6], right).wait_recv()
    remote(kvo.at[1, 1], kvo.at[2, 1], kv_sem.at[3], kv_sem.at[7], left).wait_recv()
    kp[pl.ds(3 * rows, rows), :] = pack(kvo.at[2, 0])
    vp[pl.ds(3 * rows, rows), :] = pack(kvo.at[2, 1])

    scale = 1.0 / math.sqrt(feats)
    qb = 128

    def attend(i, carry):
        q = qp[pl.ds(pl.multiple_of(i * qb, qb), qb), :]
        high = None
        for j in range(nx):
            s = dot_last(q, kp[j * rows : (j + 1) * rows, :])
            scores[:, j * rows : (j + 1) * rows] = s
            top = jnp.max(s, axis=1, keepdims=True)
            high = top if high is None else jnp.maximum(high, top)
        total = jnp.zeros((qb, 1), F32)
        acc = jnp.zeros((qb, feats), F32)
        for j in range(nx):
            e = jnp.exp((scores[:, j * rows : (j + 1) * rows] - high) * scale)
            total += jnp.sum(e, axis=1, keepdims=True)
            acc += dot(e.astype(BF16), vp[j * rows : (j + 1) * rows, :])
        o = acc / total
        att[pl.ds(i * (qb // 8), qb // 8)] = o.reshape(qb // 8, 8, feats).astype(BF16)
        return carry

    lax.fori_loop(0, rows // qb, attend, 0)
    advance(2)

    def send_back(zz, cc):
        return remote(
            att.at[2 * zz + cc], att_all.at[c, 2 * x + cc, :, head_cols(z)], back_sem.at[0], back_sem.at[1],
            {"sp": zz, "tp": 2 * x + cc},
        )

    def back_one(e, carry):
        zz = (z + e) % sp
        send_back(zz, 0).start()
        send_back(zz, 1).start()
        return carry

    lax.fori_loop(1, sp, back_one, 0)
    remote(
        att.at[2 * z + 1 - c], att_all.at[c, sib, :, head_cols(z)], back_sem.at[0], back_sem.at[1], {"tp": sib}
    ).start()
    att_all[c, t, :, head_cols(z)] = att[slot]
    advance(5)
    most = att.at[pl.ds(0, n - 1)]
    pltpu.make_async_copy(most, most, back_sem.at[1]).wait()

    def tp_gather(full, half, sems, between):
        rs = lambda i: sems.at[1, i]
        ss = lambda i: sems.at[0, i]
        tl, tr, to = 2 * xl + c, 2 * xr + c, 2 * xo + c
        sibling = {"tp": sib}

        def got(ref, i):
            remote(ref, ref, ss(i), rs(i), sibling).wait_recv()

        send(full(t), full(t), ss(0), rs(0), right)
        send(full(t), full(t), ss(1), rs(1), left)
        send(full(t), full(t), ss(2), rs(2), sibling)
        between()
        got(full(tl), 0)
        send(half(tl, 0), half(tl, 0), ss(3), rs(3), right)
        send(full(tl), full(tl), ss(4), rs(4), sibling)
        got(full(tr), 1)
        send(half(tr, 1), half(tr, 1), ss(5), rs(5), left)
        send(full(tr), full(tr), ss(6), rs(6), sibling)
        got(half(to, 0), 3)
        send(half(to, 0), half(to, 0), ss(7), rs(7), sibling)
        got(half(to, 1), 5)
        send(half(to, 1), half(to, 1), ss(8), rs(8), sibling)
        d = 1 - 2 * c
        got(full(t + d), 2)
        got(full(tl + d), 4)
        got(full(tr + d), 6)
        got(half(to + d, 0), 7)
        got(half(to + d, 1), 8)

    tp_gather(lambda i: att_all.at[:, i], lambda i, h: att_all.at[h, i], gat_sem, lambda: advance(2))
    advance(0, half + 1)

    nrow, width = mixed.shape
    mixed[...] = jnp.zeros_like(mixed)

    def project(i, carry):
        acc = jnp.zeros((nrow, width), F32)
        for u in range(4):
            h = i * 4 + u
            a = att_all[:, :, :, head_cols(h)].astype(F32).reshape(nrow, feats).astype(BF16)
            acc += dot_last(a, wo_full[h])
        mixed[...] += acc
        return carry

    lax.fori_loop(0, heads // 4, project, 0)
    res = res_ref[...].astype(F32).reshape(nrow, width)
    mix = res + mod_ref[0:1, :] * mixed[...]
    mixed[...] = mix
    local_sum = jnp.sum(mix, axis=1, keepdims=True)
    off = mix - local_sum * (1.0 / width)
    local_sq = jnp.sum(off * off, axis=1, keepdims=True)

    def as_row(col):
        return jnp.transpose(jnp.broadcast_to(col, (nrow, nrow)))[0:4, :]

    stats[t] = jnp.concatenate([as_row(local_sum), as_row(local_sq)], axis=0)
    advance(1)
    for j in range(1, tp):
        dev = (t + j) % tp
        remote(stats.at[t], stats.at[t], st_sem.at[0], st_sem.at[1], {"tp": dev}).start()
    others = stats.at[pl.ds(0, tp - 1)]
    pltpu.make_async_copy(others, others, st_sem.at[1]).wait()
    every = stats[...]
    sums, squares = every[:, 0:1, :], every[:, 4:5, :]
    mean = jnp.sum(sums, axis=0) * (1.0 / (tp * width))
    shift = sums * (1.0 / width) - mean[None]
    spread = (jnp.sum(squares, axis=0) + width * jnp.sum(shift * shift, axis=0)) * (1.0 / (tp * width))
    inv = lax.rsqrt(spread + 1e-06)

    def as_col(row):
        return jnp.transpose(jnp.broadcast_to(row, (nrow, nrow)))[:, 0:1]

    mix = mixed[...]
    normed = (mix - as_col(mean)) * as_col(inv) * (1.0 + mod_ref[2:3, :]) + mod_ref[1:2, :]
    normed_all[t] = normed.astype(BF16)
    advance(1)
    hr = nrow // 2
    tp_gather(
        lambda i: normed_all.at[i], lambda i, h: normed_all.at[i, pl.ds(h * hr, hr), :], gnm_sem, lambda: advance(1)
    )
    advance(sp)
    pushed = w2.at[1 - par, pl.ds(0, (sp - 1) * shard), :]
    pltpu.make_async_copy(pushed, pushed, pair_sem.at[1]).wait()

    ff = active.shape[1]
    for lo in range(0, ff, 256):
        hi = min(lo + 256, ff)
        acc = jnp.zeros((nrow, hi - lo), F32)
        for i in range(tp):
            acc += dot(normed_all[i], w2[0, i * width : (i + 1) * width, lo:hi])
        inner = math.sqrt(2 / math.pi) * (acc + 0.044715 * (acc * acc * acc))
        active[:, lo:hi] = (0.5 * acc * (1.0 + jnp.tanh(inner))).astype(BF16)

    def down(i):
        dev = (t + i) % tp
        block = w2[1, pl.ds(pl.multiple_of(dev * width, 16), width), :]
        return dev, dot_last(active[...], block).astype(BF16)

    waiting = None
    for i in (4, 5, 3, 2, 6, 7, 1, 0):
        dev, block = down(i)
        if i:
            part_send[dev] = block
        else:
            part_recv[t] = block
        if waiting is not None:
            remote(part_send.at[waiting], part_recv.at[t], rs_sem.at[0], rs_sem.at[1], {"tp": waiting}).start()
        waiting = dev
    seven = part_recv.at[pl.ds(0, tp - 1)]
    pltpu.make_async_copy(seven, seven, rs_sem.at[1]).wait()
    total = part_recv[0].astype(F32)
    for i in range(1, tp):
        total += part_recv[i].astype(F32)
    out = mixed[...] + mod_ref[3:4, :] * total
    out_ref[...] = out.astype(BF16).reshape(out_ref.shape)

    for d in pending:
        d.wait_send()
    pltpu.make_async_copy(rest, rest, a2a_sem.at[0]).wait()
    pltpu.make_async_copy(most, most, back_sem.at[0]).wait()
    pltpu.make_async_copy(others, others, st_sem.at[0]).wait()
    pltpu.make_async_copy(seven, seven, rs_sem.at[0]).wait()
    pltpu.make_async_copy(pushed, pushed, pair_sem.at[0]).wait()
    for a in (0, 1):
        for d in (0, 1):
            k = hops[a][d]
            ref = wo_full.at[pl.ds(0, k)] if a == 0 else w2.at[par, pl.ds(0, k * shard), :]
            pltpu.make_async_copy(ref, ref, ring_send.at[2 * a + d]).wait()


def block(sp, tp, q, k, v, residual, modulation, wo, up, dn):
    mb, tokens, inner = q.shape
    feats = inner // sp
    width = wo.shape[0]
    nrow = mb * residual.shape[1]
    shard, ff = up.shape
    nslot = 2 * sp
    rows = tokens * nslot
    dma, reg = pltpu.SemaphoreType.DMA, pltpu.SemaphoreType.REGULAR
    anyspace = pl.BlockSpec(memory_space=pl.ANY)
    vmem = pl.BlockSpec(memory_space=pltpu.VMEM)
    V = pltpu.VMEM
    return pl.pallas_call(
        functools.partial(kernel, sp, tp),
        out_shape=jax.ShapeDtypeStruct(residual.shape, BF16),
        in_specs=[anyspace] * 3 + [vmem] * 2 + [anyspace] * 3,
        out_specs=vmem,
        scratch_shapes=[
            V((3, mb, tokens, inner), BF16),
            V((3, nslot, tokens, feats), BF16),
            V((3, 2, nslot, tokens, feats), BF16),
            V((rows, feats), BF16),
            V((tp // 2 * rows, feats), BF16),
            V((tp // 2 * rows, feats), BF16),
            V((128, tp // 2 * rows), F32),
            V((nslot, tokens, feats), BF16),
            V((mb, tp, tokens, inner), BF16),
            V((sp, width, feats), BF16),
            V((2, sp * shard, ff), BF16),
            V((nrow, width), F32),
            V((tp, 8, 128), F32),
            V((tp, nrow, width), BF16),
            V((nrow, ff), BF16),
            V((tp, nrow, width), BF16),
            V((tp, nrow, width), BF16),
            dma((6,)), dma((4, sp // 2)), dma((4,)), dma((2,)), reg((1,)), reg((sp,)), dma((2,)), dma((8,)), dma((2,)),
            dma((2, 9)), dma((2, 9)), dma((2,)), dma((2,)),
        ],
        compiler_params=pltpu.CompilerParams(
            collective_id=0, has_side_effects=True, vmem_limit_bytes=60 * 1024 * 1024
        ),
    )(q, k, v, residual, modulation, wo, up, dn)


def solution(mesh):
    in_specs = (
        P("groups", ("sp", "tp"), None),
        P("groups", ("sp", "tp"), None),
        P("groups", ("sp", "tp"), None),
        P("groups", "sp", "tp"),
        P(None, "tp"),
        P("tp", "sp"),
        P("sp", "tp"),
        P("sp", "tp"),
    )
    body = functools.partial(block, mesh.shape["sp"], mesh.shape["tp"])
    return jax.shard_map(body, mesh=mesh, in_specs=in_specs, out_specs=P("groups", "sp", "tp"), check_vma=False)
```

```python
import functools
import math

import jax
import jax.numpy as jnp
from jax import lax
from jax.experimental import pallas as pl
from jax.experimental.pallas import tpu as pltpu
from jax.sharding import PartitionSpec as P

MESH = pl.DeviceIdType.MESH
F32 = jnp.float32
BF16 = jnp.bfloat16


def dot_last(a, b):
    return lax.dot_general(a, b, (((1,), (1,)), ((), ())), preferred_element_type=F32)


def dot(a, b):
    return jnp.dot(a, b, preferred_element_type=F32)


def kernel(
    sp, tp, q_hbm, k_hbm, v_hbm, res_ref, mod_ref, wo_hbm, up_hbm, dn_hbm, out_ref,
    qkv, qkvr, kvo, qp, kp, vp, scores, att, att_all, wo_full, w2, mixed, stats, normed_all,
    active, part_send, part_recv,
    local_sem, ring_recv, ring_send, pair_sem, far_sem, a2a_sem, kv_sem, back_sem, gat_sem, gnm_sem, st_sem, rs_sem,
):
    heads, feats = sp, qkvr.shape[-1]
    nx = tp // 2
    g, t, z = lax.axis_index("groups"), lax.axis_index("tp"), lax.axis_index("sp")
    x, c = t // 2, t % 2
    par = g % 2
    xr, xl, xo = (x + 1) % nx, (x + nx - 1) % nx, (x + 2) % nx
    zr, zl = (z + 1) % sp, (z + sp - 1) % sp
    sib = t + 1 - 2 * c
    pending = []

    def remote(src, dst, send, recv, dev):
        return pltpu.make_async_remote_copy(
            src_ref=src, dst_ref=dst, send_sem=send, recv_sem=recv, device_id=dev, device_id_type=MESH
        )

    def send(src, dst, s, r, dev):
        d = remote(src, dst, s, r, dev)
        d.start()
        pending.append(d)

    shard = up_hbm.shape[0]

    def w2rows(a, o):
        return w2.at[a, pl.ds(pl.multiple_of(o * shard, 16), shard), :]

    locals_w = [
        pltpu.make_async_copy(wo_hbm, wo_full.at[z], local_sem.at[0]),
        pltpu.make_async_copy(up_hbm, w2rows(0, z), local_sem.at[1]),
        pltpu.make_async_copy(dn_hbm, w2rows(1, z), local_sem.at[2]),
    ]
    locals_a = [
        pltpu.make_async_copy(r, qkv.at[i], local_sem.at[3 + i]) for i, r in enumerate((q_hbm, k_hbm, v_hbm))
    ]
    for d in locals_w + locals_a:
        d.start()

    bar = pltpu.get_barrier_semaphore()
    near = [{"tp": (t + j) % tp} for j in range(1, tp)]
    near += [{"sp": zz, "tp": 2 * x + cc} for zz in (zr, zl) for cc in (0, 1)]
    near += [{"groups": g + 1 - 2 * par}]
    for dev in near:
        pl.semaphore_signal(bar, inc=1, device_id=dev, device_id_type=MESH)
    pl.semaphore_wait(bar, len(near))

    hops = ((sp // 2 - 1, sp // 2), (sp // 2, sp // 2 - 1))

    def ring_ref(a, o):
        return wo_full.at[o] if a == 0 else w2rows(par, o)

    def ring_copy(a, d, k):
        o = (z - k + sp) % sp if d == 0 else (z + k) % sp
        return remote(
            ring_ref(a, o), ring_ref(a, o), ring_send.at[2 * a + d], ring_recv.at[2 * a + d, k],
            {"sp": zr if d == 0 else zl},
        )

    def ring_arrival(a, d, k):
        o = (z - 1 - k + 2 * sp) % sp if d == 0 else (z + 1 + k) % sp
        ref = ring_ref(a, o)
        return remote(ref, ref, ring_send.at[2 * a + d], ring_recv.at[2 * a + d, k], {"sp": zr if d == 0 else zl}), o

    def push(o):
        remote(w2rows(par, o), w2rows(par, o), pair_sem.at[0], pair_sem.at[1], {"groups": g + 1 - 2 * par}).start()

    def ring_step(a, k):
        for d in (0, 1):
            if k >= 1 and k - 1 < hops[a][d]:
                arrival, o = ring_arrival(a, d, k - 1)
                arrival.wait_recv()
                if a == 1:
                    push(o)
            if k < hops[a][d]:
                ring_copy(a, d, k).start()

    last = sp // 2
    done = [0, 0]

    def advance(n_wo=0, n_w2=0):
        for i in range(max(n_wo, n_w2)):
            for a, n in ((0, n_wo), (1, n_w2)):
                if i < n and done[a] <= last:
                    ring_step(a, done[a])
                    done[a] += 1

    for d in locals_w:
        d.wait()
    advance(1, 1)
    for d in locals_a:
        d.wait()

    slot = 2 * z + c

    def head_cols(h):
        return pl.ds(pl.multiple_of(h * feats, 128), feats)

    def send_heads(e):
        zz = (z + e + sp) % sp
        for m in (0, 1):
            remote(
                qkv.at[:, m, :, head_cols(zz)], qkvr.at[:, slot], a2a_sem.at[0], a2a_sem.at[1],
                {"sp": zz, "tp": 2 * x + m},
            ).start()

    def send_both(lo, hi):
        def one(e, carry):
            send_heads(e)
            send_heads(-e)
            return carry
        lax.fori_loop(lo, hi, one, 0)

    remote(
        qkv.at[:, 1 - c, :, head_cols(z)], qkvr.at[:, slot], a2a_sem.at[0], a2a_sem.at[1], {"tp": sib}
    ).start()
    qkvr[:, slot] = qkv[:, c, :, head_cols(z)]
    send_both(1, 2)
    reach, r = 1, 0
    while reach < sp // 2:
        for zz in ((z + reach) % sp, (z - reach + sp) % sp):
            pl.semaphore_signal(far_sem.at[r], inc=1, device_id={"sp": zz}, device_id_type=MESH)
        pl.semaphore_wait(far_sem.at[r], 2)
        send_both(reach + 1, min(2 * reach, sp // 2 - 1) + 1)
        reach, r = 2 * reach, r + 1
        if r < 4:
            advance(1, 1)
    send_heads(sp // 2)
    advance(0, 4)
    n = 2 * sp
    rest = qkvr.at[:, pl.ds(0, n - 1)]
    pltpu.make_async_copy(rest, rest, a2a_sem.at[1]).wait()

    own_kv = qkvr.at[pl.ds(1, 2)]
    right, left = {"tp": 2 * xr + c}, {"tp": 2 * xl + c}
    send(own_kv, kvo.at[0], kv_sem.at[0], kv_sem.at[4], right)
    send(own_kv, kvo.at[1], kv_sem.at[1], kv_sem.at[5], left)
    advance(1, 1)

    def pack(ref):
        v = ref[...].astype(F32)
        return v.reshape(v.shape[0] * v.shape[1], v.shape[2]).astype(BF16)

    rows = 8 * n
    qp[...] = pack(qkvr.at[0])
    kp[pl.ds(0, rows), :] = pack(qkvr.at[1])
    vp[pl.ds(0, rows), :] = pack(qkvr.at[2])
    remote(own_kv, kvo.at[0], kv_sem.at[0], kv_sem.at[4], right).wait_recv()
    send(kvo.at[0, 0], kvo.at[2, 0], kv_sem.at[2], kv_sem.at[6], right)
    advance(1, 1)
    remote(own_kv, kvo.at[1], kv_sem.at[1], kv_sem.at[5], left).wait_recv()
    send(kvo.at[1, 1], kvo.at[2, 1], kv_sem.at[3], kv_sem.at[7], left)
    for j in (0, 1):
        kp[pl.ds((1 + j) * rows, rows), :] = pack(kvo.at[j, 0])
        vp[pl.ds((1 + j) * rows, rows), :] = pack(kvo.at[j, 1])
    advance(1, 1)
    remote(kvo.at[0, 0], kvo.at[2, 0], kv_sem.at[2], kv_sem.at[6], right).wait_recv()
    remote(kvo.at[1, 1], kvo.at[2, 1], kv_sem.at[3], kv_sem.at[7], left).wait_recv()
    kp[pl.ds(3 * rows, rows), :] = pack(kvo.at[2, 0])
    vp[pl.ds(3 * rows, rows), :] = pack(kvo.at[2, 1])

    scale = 1.0 / math.sqrt(feats)
    qb = 128

    def attend(i, carry):
        q = qp[pl.ds(pl.multiple_of(i * qb, qb), qb), :]
        high = None
        for j in range(nx):
            s = dot_last(q, kp[j * rows : (j + 1) * rows, :])
            scores[:, j * rows : (j + 1) * rows] = s
            top = jnp.max(s, axis=1, keepdims=True)
            high = top if high is None else jnp.maximum(high, top)
        total = jnp.zeros((qb, 1), F32)
        acc = jnp.zeros((qb, feats), F32)
        for j in range(nx):
            e = jnp.exp((scores[:, j * rows : (j + 1) * rows] - high) * scale)
            total += jnp.sum(e, axis=1, keepdims=True)
            acc += dot(e.astype(BF16), vp[j * rows : (j + 1) * rows, :])
        o = acc / total
        att[pl.ds(i * (qb // 8), qb // 8)] = o.reshape(qb // 8, 8, feats).astype(BF16)
        return carry

    lax.fori_loop(0, rows // qb, attend, 0)
    advance(1, 1)

    def send_back(zz, cc):
        return remote(
            att.at[2 * zz + cc], att_all.at[c, 2 * x + cc, :, head_cols(z)], back_sem.at[0], back_sem.at[1],
            {"sp": zz, "tp": 2 * x + cc},
        )

    def back_one(e, carry):
        zz = (z + e) % sp
        send_back(zz, 0).start()
        send_back(zz, 1).start()
        return carry

    lax.fori_loop(1, sp, back_one, 0)
    remote(
        att.at[2 * z + 1 - c], att_all.at[c, sib, :, head_cols(z)], back_sem.at[0], back_sem.at[1], {"tp": sib}
    ).start()
    att_all[c, t, :, head_cols(z)] = att[slot]
    advance(2, 2)
    most = att.at[pl.ds(0, n - 1)]
    pltpu.make_async_copy(most, most, back_sem.at[1]).wait()

    def tp_gather(full, half, sems, between):
        rs = lambda i: sems.at[1, i]
        ss = lambda i: sems.at[0, i]
        tl, tr, to = 2 * xl + c, 2 * xr + c, 2 * xo + c
        sibling = {"tp": sib}

        def got(ref, i):
            remote(ref, ref, ss(i), rs(i), sibling).wait_recv()

        send(full(t), full(t), ss(0), rs(0), right)
        send(full(t), full(t), ss(1), rs(1), left)
        send(full(t), full(t), ss(2), rs(2), sibling)
        between()
        got(full(tl), 0)
        send(half(tl, 0), half(tl, 0), ss(3), rs(3), right)
        send(full(tl), full(tl), ss(4), rs(4), sibling)
        got(full(tr), 1)
        send(half(tr, 1), half(tr, 1), ss(5), rs(5), left)
        send(full(tr), full(tr), ss(6), rs(6), sibling)
        between()
        got(half(to, 0), 3)
        send(half(to, 0), half(to, 0), ss(7), rs(7), sibling)
        got(half(to, 1), 5)
        send(half(to, 1), half(to, 1), ss(8), rs(8), sibling)
        d = 1 - 2 * c
        got(full(t + d), 2)
        got(full(tl + d), 4)
        got(full(tr + d), 6)
        got(half(to + d, 0), 7)
        got(half(to + d, 1), 8)

    tp_gather(lambda i: att_all.at[:, i], lambda i, h: att_all.at[h, i], gat_sem, lambda: advance(3, 1))
    advance(sp, 0)

    nrow, width = mixed.shape
    mixed[...] = jnp.zeros_like(mixed)

    def project(i, carry):
        acc = jnp.zeros((nrow, width), F32)
        for u in range(4):
            h = i * 4 + u
            a = att_all[:, :, :, head_cols(h)].astype(F32).reshape(nrow, feats).astype(BF16)
            acc += dot_last(a, wo_full[h])
        mixed[...] += acc
        return carry

    lax.fori_loop(0, heads // 4, project, 0)
    res = res_ref[...].astype(F32).reshape(nrow, width)
    mix = res + mod_ref[0:1, :] * mixed[...]
    mixed[...] = mix
    local_sum = jnp.sum(mix, axis=1, keepdims=True)
    off = mix - local_sum * (1.0 / width)
    local_sq = jnp.sum(off * off, axis=1, keepdims=True)

    def as_row(col):
        return jnp.transpose(jnp.broadcast_to(col, (nrow, nrow)))[0:4, :]

    stats[t] = jnp.concatenate([as_row(local_sum), as_row(local_sq)], axis=0)
    advance(0, 1)
    for j in range(1, tp):
        dev = (t + j) % tp
        remote(stats.at[t], stats.at[t], st_sem.at[0], st_sem.at[1], {"tp": dev}).start()
    others = stats.at[pl.ds(0, tp - 1)]
    pltpu.make_async_copy(others, others, st_sem.at[1]).wait()
    every = stats[...]
    sums, squares = every[:, 0:1, :], every[:, 4:5, :]
    mean = jnp.sum(sums, axis=0) * (1.0 / (tp * width))
    shift = sums * (1.0 / width) - mean[None]
    spread = (jnp.sum(squares, axis=0) + width * jnp.sum(shift * shift, axis=0)) * (1.0 / (tp * width))
    inv = lax.rsqrt(spread + 1e-06)

    def as_col(row):
        return jnp.transpose(jnp.broadcast_to(row, (nrow, nrow)))[:, 0:1]

    mix = mixed[...]
    normed = (mix - as_col(mean)) * as_col(inv) * (1.0 + mod_ref[2:3, :]) + mod_ref[1:2, :]
    normed_all[t] = normed.astype(BF16)
    advance(0, 1)
    hr = nrow // 2
    tp_gather(
        lambda i: normed_all.at[i], lambda i, h: normed_all.at[i, pl.ds(h * hr, hr), :], gnm_sem, lambda: advance(0, 1)
    )
    advance(0, sp)
    pushed = w2.at[1 - par, pl.ds(0, (sp - 1) * shard), :]
    pltpu.make_async_copy(pushed, pushed, pair_sem.at[1]).wait()

    ff = active.shape[1]
    for lo in range(0, ff, 256):
        hi = min(lo + 256, ff)
        acc = jnp.zeros((nrow, hi - lo), F32)
        for i in range(tp):
            acc += dot(normed_all[i], w2[0, i * width : (i + 1) * width, lo:hi])
        inner = math.sqrt(2 / math.pi) * (acc + 0.044715 * (acc * acc * acc))
        active[:, lo:hi] = (0.5 * acc * (1.0 + jnp.tanh(inner))).astype(BF16)

    def down(i):
        dev = (t + i) % tp
        block = w2[1, pl.ds(pl.multiple_of(dev * width, 16), width), :]
        return dev, dot_last(active[...], block).astype(BF16)

    waiting = None
    for i in (4, 5, 3, 2, 6, 7, 1, 0):
        dev, block = down(i)
        if i:
            part_send[dev] = block
        else:
            part_recv[t] = block
        if waiting is not None:
            remote(part_send.at[waiting], part_recv.at[t], rs_sem.at[0], rs_sem.at[1], {"tp": waiting}).start()
        waiting = dev
    seven = part_recv.at[pl.ds(0, tp - 1)]
    pltpu.make_async_copy(seven, seven, rs_sem.at[1]).wait()
    total = part_recv[0].astype(F32)
    for i in range(1, tp):
        total += part_recv[i].astype(F32)
    out = mixed[...] + mod_ref[3:4, :] * total
    out_ref[...] = out.astype(BF16).reshape(out_ref.shape)

    for d in pending:
        d.wait_send()
    pltpu.make_async_copy(rest, rest, a2a_sem.at[0]).wait()
    pltpu.make_async_copy(most, most, back_sem.at[0]).wait()
    pltpu.make_async_copy(others, others, st_sem.at[0]).wait()
    pltpu.make_async_copy(seven, seven, rs_sem.at[0]).wait()
    pltpu.make_async_copy(pushed, pushed, pair_sem.at[0]).wait()
    for a in (0, 1):
        for d in (0, 1):
            k = hops[a][d]
            ref = wo_full.at[pl.ds(0, k)] if a == 0 else w2.at[par, pl.ds(0, k * shard), :]
            pltpu.make_async_copy(ref, ref, ring_send.at[2 * a + d]).wait()


def block(sp, tp, q, k, v, residual, modulation, wo, up, dn):
    mb, tokens, inner = q.shape
    feats = inner // sp
    width = wo.shape[0]
    nrow = mb * residual.shape[1]
    shard, ff = up.shape
    nslot = 2 * sp
    rows = tokens * nslot
    dma, reg = pltpu.SemaphoreType.DMA, pltpu.SemaphoreType.REGULAR
    anyspace = pl.BlockSpec(memory_space=pl.ANY)
    vmem = pl.BlockSpec(memory_space=pltpu.VMEM)
    V = pltpu.VMEM
    return pl.pallas_call(
        functools.partial(kernel, sp, tp),
        out_shape=jax.ShapeDtypeStruct(residual.shape, BF16),
        in_specs=[anyspace] * 3 + [vmem] * 2 + [anyspace] * 3,
        out_specs=vmem,
        scratch_shapes=[
            V((3, mb, tokens, inner), BF16),
            V((3, nslot, tokens, feats), BF16),
            V((3, 2, nslot, tokens, feats), BF16),
            V((rows, feats), BF16),
            V((tp // 2 * rows, feats), BF16),
            V((tp // 2 * rows, feats), BF16),
            V((128, tp // 2 * rows), F32),
            V((nslot, tokens, feats), BF16),
            V((mb, tp, tokens, inner), BF16),
            V((sp, width, feats), BF16),
            V((2, sp * shard, ff), BF16),
            V((nrow, width), F32),
            V((tp, 8, 128), F32),
            V((tp, nrow, width), BF16),
            V((nrow, ff), BF16),
            V((tp, nrow, width), BF16),
            V((tp, nrow, width), BF16),
            dma((6,)), dma((4, sp // 2)), dma((4,)), dma((2,)), reg((8,)), dma((2,)), dma((8,)), dma((2,)),
            dma((2, 9)), dma((2, 9)), dma((2,)), dma((2,)),
        ],
        compiler_params=pltpu.CompilerParams(
            collective_id=0, has_side_effects=True, vmem_limit_bytes=60 * 1024 * 1024
        ),
    )(q, k, v, residual, modulation, wo, up, dn)


def solution(mesh):
    in_specs = (
        P("groups", ("sp", "tp"), None),
        P("groups", ("sp", "tp"), None),
        P("groups", ("sp", "tp"), None),
        P("groups", "sp", "tp"),
        P(None, "tp"),
        P("tp", "sp"),
        P("sp", "tp"),
        P("sp", "tp"),
    )
    body = functools.partial(block, mesh.shape["sp"], mesh.shape["tp"])
    return jax.shard_map(body, mesh=mesh, in_specs=in_specs, out_specs=P("groups", "sp", "tp"), check_vma=False)
```

```python
import functools
import math

import jax
import jax.numpy as jnp
from jax import lax
from jax.experimental import pallas as pl
from jax.experimental.pallas import tpu as pltpu
from jax.sharding import PartitionSpec as P

MESH = pl.DeviceIdType.MESH
F32 = jnp.float32
BF16 = jnp.bfloat16


def dot_last(a, b):
    return lax.dot_general(a, b, (((1,), (1,)), ((), ())), preferred_element_type=F32)


def dot(a, b):
    return jnp.dot(a, b, preferred_element_type=F32)


def kernel(
    sp, tp, q_hbm, k_hbm, v_hbm, res_ref, mod_ref, wo_hbm, up_hbm, dn_hbm, out_ref,
    qkv, qkvr, kvo, qp, kp, vp, scores, att, att_all, wo_full, w2, mixed, stats, normed_all,
    active, part_send, part_out, sib_recv, part_recv,
    local_sem, ring_recv, ring_send, pair_sem, far_sem, a2a_sem, kv_sem, back_sem, gat_sem, gnm_sem, st_sem, rs_sem, sib_sem,
):
    heads, feats = sp, qkvr.shape[-1]
    nx = tp // 2
    g, t, z = lax.axis_index("groups"), lax.axis_index("tp"), lax.axis_index("sp")
    x, c = t // 2, t % 2
    par = g % 2
    xr, xl, xo = (x + 1) % nx, (x + nx - 1) % nx, (x + 2) % nx
    zr, zl = (z + 1) % sp, (z + sp - 1) % sp
    sib = t + 1 - 2 * c
    pending = []

    def remote(src, dst, send, recv, dev):
        return pltpu.make_async_remote_copy(
            src_ref=src, dst_ref=dst, send_sem=send, recv_sem=recv, device_id=dev, device_id_type=MESH
        )

    def send(src, dst, s, r, dev):
        d = remote(src, dst, s, r, dev)
        d.start()
        pending.append(d)

    shard = up_hbm.shape[0]

    def w2rows(a, o):
        return w2.at[a, pl.ds(pl.multiple_of(o * shard, 16), shard), :]

    locals_w = [
        pltpu.make_async_copy(wo_hbm, wo_full.at[z], local_sem.at[0]),
        pltpu.make_async_copy(up_hbm, w2rows(0, z), local_sem.at[1]),
        pltpu.make_async_copy(dn_hbm, w2rows(1, z), local_sem.at[2]),
    ]
    locals_a = [
        pltpu.make_async_copy(r, qkv.at[i], local_sem.at[3 + i]) for i, r in enumerate((q_hbm, k_hbm, v_hbm))
    ]
    for d in locals_w + locals_a:
        d.start()

    bar = pltpu.get_barrier_semaphore()
    near = [{"tp": (t + j) % tp} for j in range(1, tp)]
    near += [{"sp": zz, "tp": 2 * x + cc} for zz in (zr, zl) for cc in (0, 1)]
    near += [{"groups": g + 1 - 2 * par}]
    for dev in near:
        pl.semaphore_signal(bar, inc=1, device_id=dev, device_id_type=MESH)
    pl.semaphore_wait(bar, len(near))

    hops = ((sp // 2 - 1, sp // 2), (sp // 2, sp // 2 - 1))

    quarter = wo_hbm.shape[0] // 4

    def ring_ref(a, o):
        if a == 0:
            return wo_full.at[o, pl.ds(pl.multiple_of(par * quarter, 16), 3 * quarter), :]
        return w2rows(par, o)

    def ring_copy(a, d, k):
        o = (z - k + sp) % sp if d == 0 else (z + k) % sp
        return remote(
            ring_ref(a, o), ring_ref(a, o), ring_send.at[2 * a + d], ring_recv.at[2 * a + d, k],
            {"sp": zr if d == 0 else zl},
        )

    def ring_arrival(a, d, k):
        o = (z - 1 - k + 2 * sp) % sp if d == 0 else (z + 1 + k) % sp
        ref = ring_ref(a, o)
        return remote(ref, ref, ring_send.at[2 * a + d], ring_recv.at[2 * a + d, k], {"sp": zr if d == 0 else zl}), o

    def push(a, o):
        ref = wo_full.at[o, pl.ds(pl.multiple_of(par * 3 * quarter, 16), quarter), :] if a == 0 else w2rows(par, o)
        remote(ref, ref, pair_sem.at[a, 0], pair_sem.at[a, 1], {"groups": g + 1 - 2 * par}).start()

    def ring_step(a, k):
        for d in (0, 1):
            if k >= 1 and k - 1 < hops[a][d]:
                arrival, o = ring_arrival(a, d, k - 1)
                arrival.wait_recv()
                push(a, o)
            if k < hops[a][d]:
                ring_copy(a, d, k).start()

    last = sp // 2
    done = [0, 0]

    def advance(n_wo=0, n_w2=0):
        for i in range(max(n_wo, n_w2)):
            for a, n in ((0, n_wo), (1, n_w2)):
                if i < n and done[a] <= last:
                    ring_step(a, done[a])
                    done[a] += 1

    for d in locals_w:
        d.wait()
    advance(1, 1)
    for d in locals_a:
        d.wait()

    slot = 2 * z + c

    def head_cols(h):
        return pl.ds(pl.multiple_of(h * feats, 128), feats)

    def send_heads(e):
        zz = (z + e + sp) % sp
        for m in (0, 1):
            remote(
                qkv.at[:, m, :, head_cols(zz)], qkvr.at[:, slot], a2a_sem.at[0], a2a_sem.at[1],
                {"sp": zz, "tp": 2 * x + m},
            ).start()

    def send_both(lo, hi):
        def one(i, carry):
            e = hi - 1 - i
            send_heads(e)
            send_heads(-e)
            return carry
        lax.fori_loop(0, hi - lo, one, 0)

    remote(
        qkv.at[:, 1 - c, :, head_cols(z)], qkvr.at[:, slot], a2a_sem.at[0], a2a_sem.at[1], {"tp": sib}
    ).start()
    qkvr[:, slot] = qkv[:, c, :, head_cols(z)]
    send_both(1, 2)
    reach, r = 1, 0
    while reach < sp // 2:
        for zz in ((z + reach) % sp, (z - reach + sp) % sp):
            pl.semaphore_signal(far_sem.at[r], inc=1, device_id={"sp": zz}, device_id_type=MESH)
        pl.semaphore_wait(far_sem.at[r], 2)
        if 2 * reach == sp // 2:
            send_heads(sp // 2)
        send_both(reach + 1, min(2 * reach, sp // 2 - 1) + 1)
        reach, r = 2 * reach, r + 1
        if r < 4:
            advance(1, 1)
    advance(0, 2)
    n = 2 * sp
    rest = qkvr.at[:, pl.ds(0, n - 1)]
    pltpu.make_async_copy(rest, rest, a2a_sem.at[1]).wait()

    own_kv = qkvr.at[pl.ds(1, 2)]
    right, left = {"tp": 2 * xr + c}, {"tp": 2 * xl + c}
    send(own_kv, kvo.at[0], kv_sem.at[0], kv_sem.at[4], right)
    send(own_kv, kvo.at[1], kv_sem.at[1], kv_sem.at[5], left)
    advance(1, 1)

    def pack(ref):
        v = ref[...].astype(F32)
        return v.reshape(v.shape[0] * v.shape[1], v.shape[2]).astype(BF16)

    rows = 8 * n
    qp[...] = pack(qkvr.at[0])
    kp[pl.ds(0, rows), :] = pack(qkvr.at[1])
    vp[pl.ds(0, rows), :] = pack(qkvr.at[2])
    remote(own_kv, kvo.at[0], kv_sem.at[0], kv_sem.at[4], right).wait_recv()
    send(kvo.at[0, 0], kvo.at[2, 0], kv_sem.at[2], kv_sem.at[6], right)
    advance(1, 1)
    remote(own_kv, kvo.at[1], kv_sem.at[1], kv_sem.at[5], left).wait_recv()
    send(kvo.at[1, 1], kvo.at[2, 1], kv_sem.at[3], kv_sem.at[7], left)
    for j in (0, 1):
        kp[pl.ds((1 + j) * rows, rows), :] = pack(kvo.at[j, 0])
        vp[pl.ds((1 + j) * rows, rows), :] = pack(kvo.at[j, 1])
    advance(1, 1)
    remote(kvo.at[0, 0], kvo.at[2, 0], kv_sem.at[2], kv_sem.at[6], right).wait_recv()
    remote(kvo.at[1, 1], kvo.at[2, 1], kv_sem.at[3], kv_sem.at[7], left).wait_recv()
    kp[pl.ds(3 * rows, rows), :] = pack(kvo.at[2, 0])
    vp[pl.ds(3 * rows, rows), :] = pack(kvo.at[2, 1])

    scale = 1.0 / math.sqrt(feats)
    qb = 128

    def attend(i, carry):
        q = qp[pl.ds(pl.multiple_of(i * qb, qb), qb), :]
        high = None
        for j in range(nx):
            s = dot_last(q, kp[j * rows : (j + 1) * rows, :])
            scores[:, j * rows : (j + 1) * rows] = s
            top = jnp.max(s, axis=1, keepdims=True)
            high = top if high is None else jnp.maximum(high, top)
        total = jnp.zeros((qb, 1), F32)
        acc = jnp.zeros((qb, feats), F32)
        for j in range(nx):
            e = jnp.exp((scores[:, j * rows : (j + 1) * rows] - high) * scale)
            total += jnp.sum(e, axis=1, keepdims=True)
            acc += dot(e.astype(BF16), vp[j * rows : (j + 1) * rows, :])
        o = acc / total
        att[pl.ds(i * (qb // 8), qb // 8)] = o.reshape(qb // 8, 8, feats).astype(BF16)
        return carry

    lax.fori_loop(0, rows // qb, attend, 0)

    def send_back(zz, cc):
        return remote(
            att.at[2 * zz + cc], att_all.at[c, 2 * x + cc, :, head_cols(z)], back_sem.at[0], back_sem.at[1],
            {"sp": zz, "tp": 2 * x + cc},
        )

    def back_one(i, carry):
        for zz in ((z + half - i) % sp, (z + half + i) % sp):
            send_back(zz, 0).start()
            send_back(zz, 1).start()
        return carry

    half = sp // 2
    send_back((z + half) % sp, 0).start()
    send_back((z + half) % sp, 1).start()
    lax.fori_loop(1, half, back_one, 0)
    remote(
        att.at[2 * z + 1 - c], att_all.at[c, sib, :, head_cols(z)], back_sem.at[0], back_sem.at[1], {"tp": sib}
    ).start()
    att_all[c, t, :, head_cols(z)] = att[slot]
    advance(3, 3)
    most = att.at[pl.ds(0, n - 1)]
    pltpu.make_async_copy(most, most, back_sem.at[1]).wait()

    def tp_gather(full, half, sems, between):
        rs = lambda i: sems.at[1, i]
        ss = lambda i: sems.at[0, i]
        tl, tr, to = 2 * xl + c, 2 * xr + c, 2 * xo + c
        sibling = {"tp": sib}

        def got(ref, i):
            remote(ref, ref, ss(i), rs(i), sibling).wait_recv()

        send(full(t), full(t), ss(0), rs(0), right)
        send(full(t), full(t), ss(1), rs(1), left)
        send(full(t), full(t), ss(2), rs(2), sibling)
        between()
        got(full(tl), 0)
        send(half(tl, 0), half(tl, 0), ss(3), rs(3), right)
        send(full(tl), full(tl), ss(4), rs(4), sibling)
        got(full(tr), 1)
        send(half(tr, 1), half(tr, 1), ss(5), rs(5), left)
        send(full(tr), full(tr), ss(6), rs(6), sibling)
        between()
        got(half(to, 0), 3)
        send(half(to, 0), half(to, 0), ss(7), rs(7), sibling)
        got(half(to, 1), 5)
        send(half(to, 1), half(to, 1), ss(8), rs(8), sibling)
        d = 1 - 2 * c
        got(full(t + d), 2)
        got(full(tl + d), 4)
        got(full(tr + d), 6)
        got(half(to + d, 0), 7)
        got(half(to + d, 1), 8)

    tp_gather(lambda i: att_all.at[:, i], lambda i, h: att_all.at[h, i], gat_sem, lambda: advance(3, 1))
    advance(sp, 0)
    pushed_wo = wo_full.at[pl.ds(0, sp - 1), pl.ds(0, quarter), :]
    pltpu.make_async_copy(pushed_wo, pushed_wo, pair_sem.at[0, 1]).wait()

    nrow, width = mixed.shape
    mixed[...] = jnp.zeros_like(mixed)

    def project(i, carry):
        acc = jnp.zeros((nrow, width), F32)
        for u in range(4):
            h = i * 4 + u
            a = att_all[:, :, :, head_cols(h)].astype(F32).reshape(nrow, feats).astype(BF16)
            acc += dot_last(a, wo_full[h])
        mixed[...] += acc
        return carry

    lax.fori_loop(0, heads // 4, project, 0)
    res = res_ref[...].astype(F32).reshape(nrow, width)
    mix = res + mod_ref[0:1, :] * mixed[...]
    mixed[...] = mix
    local_sum = jnp.sum(mix, axis=1, keepdims=True)
    off = mix - local_sum * (1.0 / width)
    local_sq = jnp.sum(off * off, axis=1, keepdims=True)

    def as_row(col):
        return jnp.transpose(jnp.broadcast_to(col, (nrow, nrow)))[0:4, :]

    stats[t] = jnp.concatenate([as_row(local_sum), as_row(local_sq)], axis=0)
    advance(0, 1)
    for j in range(1, tp):
        dev = (t + j) % tp
        remote(stats.at[t], stats.at[t], st_sem.at[0], st_sem.at[1], {"tp": dev}).start()
    others = stats.at[pl.ds(0, tp - 1)]
    pltpu.make_async_copy(others, others, st_sem.at[1]).wait()
    every = stats[...]
    sums, squares = every[:, 0:1, :], every[:, 4:5, :]
    mean = jnp.sum(sums, axis=0) * (1.0 / (tp * width))
    shift = sums * (1.0 / width) - mean[None]
    spread = (jnp.sum(squares, axis=0) + width * jnp.sum(shift * shift, axis=0)) * (1.0 / (tp * width))
    inv = lax.rsqrt(spread + 1e-06)

    def as_col(row):
        return jnp.transpose(jnp.broadcast_to(row, (nrow, nrow)))[:, 0:1]

    mix = mixed[...]
    normed = (mix - as_col(mean)) * as_col(inv) * (1.0 + mod_ref[2:3, :]) + mod_ref[1:2, :]
    normed_all[t] = normed.astype(BF16)
    advance(0, 1)
    hr = nrow // 2
    tp_gather(
        lambda i: normed_all.at[i], lambda i, h: normed_all.at[i, pl.ds(h * hr, hr), :], gnm_sem, lambda: advance(0, 1)
    )
    advance(0, sp)
    pushed = w2.at[1 - par, pl.ds(0, (sp - 1) * shard), :]
    pltpu.make_async_copy(pushed, pushed, pair_sem.at[1, 1]).wait()

    ff = active.shape[1]
    for lo in range(0, ff, 256):
        hi = min(lo + 256, ff)
        acc = jnp.zeros((nrow, hi - lo), F32)
        for i in range(tp):
            acc += dot(normed_all[i], w2[0, i * width : (i + 1) * width, lo:hi])
        inner = math.sqrt(2 / math.pi) * (acc + 0.044715 * (acc * acc * acc))
        active[:, lo:hi] = (0.5 * acc * (1.0 + jnp.tanh(inner))).astype(BF16)

    def down(tgt):
        return dot_last(active[...], w2[1, pl.ds(pl.multiple_of(tgt * width, 16), width), :])

    order = (xo, xr, xl, x)
    to_sib = [remote(part_send.at[i], sib_recv.at[i], sib_sem.at[0, i], sib_sem.at[1, i], {"tp": sib}) for i in range(4)]
    for i, xx in enumerate(order):
        part_send[i] = down(2 * xx + 1 - c).astype(BF16)
        if i:
            to_sib[i - 1].start()
    total = down(2 * xo + c)
    to_sib[3].start()
    for i, seat in ((0, 0), (1, 2), (2, 1)):
        to_sib[i].wait_recv()
        part_out[i] = (total + sib_recv[i].astype(F32)).astype(BF16)
        total = down(2 * order[i + 1] + c)
        remote(part_out.at[i], part_recv.at[seat], rs_sem.at[0], rs_sem.at[1], {"tp": 2 * order[i] + c}).start()
    to_sib[3].wait_recv()
    total += sib_recv[3].astype(F32)
    three = part_recv.at[pl.ds(0, 3)]
    pltpu.make_async_copy(three, three, rs_sem.at[1]).wait()
    for i in range(3):
        total += part_recv[i].astype(F32)
    out = mixed[...] + mod_ref[3:4, :] * total
    out_ref[...] = out.astype(BF16).reshape(out_ref.shape)

    for d in pending:
        d.wait_send()
    pltpu.make_async_copy(rest, rest, a2a_sem.at[0]).wait()
    pltpu.make_async_copy(most, most, back_sem.at[0]).wait()
    pltpu.make_async_copy(others, others, st_sem.at[0]).wait()
    pltpu.make_async_copy(three, three, rs_sem.at[0]).wait()
    for d in to_sib:
        d.wait_send()
    pltpu.make_async_copy(pushed, pushed, pair_sem.at[1, 0]).wait()
    pltpu.make_async_copy(pushed_wo, pushed_wo, pair_sem.at[0, 0]).wait()
    for a in (0, 1):
        for d in (0, 1):
            k = hops[a][d]
            ref = wo_full.at[pl.ds(0, k), pl.ds(0, 3 * quarter), :] if a == 0 else w2.at[par, pl.ds(0, k * shard), :]
            pltpu.make_async_copy(ref, ref, ring_send.at[2 * a + d]).wait()


def block(sp, tp, q, k, v, residual, modulation, wo, up, dn):
    mb, tokens, inner = q.shape
    feats = inner // sp
    width = wo.shape[0]
    nrow = mb * residual.shape[1]
    shard, ff = up.shape
    nslot = 2 * sp
    rows = tokens * nslot
    dma, reg = pltpu.SemaphoreType.DMA, pltpu.SemaphoreType.REGULAR
    anyspace = pl.BlockSpec(memory_space=pl.ANY)
    vmem = pl.BlockSpec(memory_space=pltpu.VMEM)
    V = pltpu.VMEM
    return pl.pallas_call(
        functools.partial(kernel, sp, tp),
        out_shape=jax.ShapeDtypeStruct(residual.shape, BF16),
        in_specs=[anyspace] * 3 + [vmem] * 2 + [anyspace] * 3,
        out_specs=vmem,
        scratch_shapes=[
            V((3, mb, tokens, inner), BF16),
            V((3, nslot, tokens, feats), BF16),
            V((3, 2, nslot, tokens, feats), BF16),
            V((rows, feats), BF16),
            V((tp // 2 * rows, feats), BF16),
            V((tp // 2 * rows, feats), BF16),
            V((128, tp // 2 * rows), F32),
            V((nslot, tokens, feats), BF16),
            V((mb, tp, tokens, inner), BF16),
            V((sp, width, feats), BF16),
            V((2, sp * shard, ff), BF16),
            V((nrow, width), F32),
            V((tp, 8, 128), F32),
            V((tp, nrow, width), BF16),
            V((nrow, ff), BF16),
            V((4, nrow, width), BF16),
            V((3, nrow, width), BF16),
            V((4, nrow, width), BF16),
            V((3, nrow, width), BF16),
            dma((6,)), dma((4, sp // 2)), dma((4,)), dma((2, 2)), reg((8,)), dma((2,)), dma((8,)), dma((2,)),
            dma((2, 9)), dma((2, 9)), dma((2,)), dma((2,)), dma((2, 4)),
        ],
        compiler_params=pltpu.CompilerParams(
            collective_id=0, has_side_effects=True, vmem_limit_bytes=60 * 1024 * 1024
        ),
    )(q, k, v, residual, modulation, wo, up, dn)


def solution(mesh):
    in_specs = (
        P("groups", ("sp", "tp"), None),
        P("groups", ("sp", "tp"), None),
        P("groups", ("sp", "tp"), None),
        P("groups", "sp", "tp"),
        P(None, "tp"),
        P("tp", "sp"),
        P("sp", "tp"),
        P("sp", "tp"),
    )
    body = functools.partial(block, mesh.shape["sp"], mesh.shape["tp"])
    return jax.shard_map(body, mesh=mesh, in_specs=in_specs, out_specs=P("groups", "sp", "tp"), check_vma=False)
```
